32 devices in a mesh: seq: 4 (over z), head: 8 (over y, x, core).
Axes of the slice: x: 2, y: 2, z: 4, core: 2. Of those that a mesh axis runs over, the one named last changes fastest.
Arguments:
- queries: float32 [2048, 4096], P('seq', 'head'), may hold values from -6 to 6
- key_rows: float32 [2048, 4096], P('seq', 'head'), may hold values from -6 to 6
- values: float32 [2048, 4096], P('seq', 'head'), may hold values from -6 to 6
- out_weight: bfloat16 [4096, 2048], P('head'), may hold values from -0.09375 to 0.09375
- expert_ids: int32 [2048, 8], P(('seq', 'head')), may hold values from 0 to 31, all different within a row; in each aligned block of 64 rows (0 to 63, 64 to 127, ...) at most 32 rows name the same one
- gate_ints: int32 [2048, 8], P(('seq', 'head')), may hold values from 1 to 1023
- w_gate: bfloat16 [32, 2048, 768], P(('seq', 'head')), may hold values from -0.125 to 0.125
- w_up: bfloat16 [32, 2048, 768], P(('seq', 'head')), may hold values from -0.125 to 0.125
- w_down: bfloat16 [32, 768, 2048], P(('seq', 'head')), may hold values from -0.21875 to 0.21875
Outputs:
- layer_out: float32 [2048, 2048], P(('seq', 'head'))
The draws below stay inside these ranges and needn't reach their ends.
Inputs may be any that keep to these rules, and one draw needn't show every extreme that they name: `expert_ids`: each row names 8 different experts. Within the rows of one device (aligned blocks of 64 rows) no expert is named more than 32 times, a bound that some block reaches.
All inputs are finite; a program needn't handle non-finite values.
Results may differ from the reference program's by a relative error of at most 0.017.
Values may be sent and summed in bfloat16 or wider, within the bound.
No kernel may reach another device: no remote copies, remote signals or barrier semaphores. Data moves between devices by JAX's collectives and lax.ppermute only.
A program may use at most 128 MiB of HBM per device.

```python
import math
import jax
import jax.numpy as jnp
import numpy as np
from jax import lax

D = 2048
FF = 768
HEADS = 32
DH = 128
TOP = 8
TOK_DEV = 64
EXPERTS = 32
LENGTH = 2048
TOKENS = 2048
CAP = 32
N_SEQ = 4
N_HEAD = 8


def set_ends(values, stream_key, low, top_value):
    place = [jax.random.randint(jax.random.fold_in(stream_key, axis), (), 0, length) for axis, length in enumerate(values.shape)]
    widest = values.shape.index(max(values.shape))
    next_to = place[:widest] + [(place[widest] + 1) % values.shape[widest]] + place[widest + 1:]
    return values.at[tuple(place)].set(low).at[tuple(next_to)].set(top_value)


def steps_of(key, shape, cuts, least, top_value):
    gain = 1.0
    for position, parts in cuts:
        heights = jax.random.uniform(jax.random.fold_in(jax.random.fold_in(key, 6), position), (parts,), jnp.float32, least / len(cuts), top_value / len(cuts))
        gain = gain * jnp.repeat(jnp.exp(heights), shape[position] // parts).reshape((-1,) + (1,) * (len(shape) - 1 - position))
    return gain


def deal_out(rng, own, number, rows, number_of, top, reach, skew):
    order = jax.random.permutation(rng, number_of)
    heavy_load, common = load_shares(number_of, rows * top, reach, skew, True), load_shares(number_of, rows * top, reach, skew, False)
    places = jnp.arange(number_of)

    def named(sizes, turn):
        used = int((sizes > 0).sum())
        fixed = max(1, used // 4)
        moved = fixed + (places - fixed + turn * (used - fixed)) % max(1, number_of - fixed)
        return jnp.zeros((number_of,), jnp.int32).at[order[jnp.where(places < fixed, places, moved)]].set(jnp.asarray(sizes, jnp.int32))

    sizes = jnp.where(number % 4 == 0, named(heavy_load, number // 4), named(common, number - number // 4 - 1))
    mixed = jax.random.permutation(jax.random.fold_in(own, 3), number_of)
    giver, receiver = mixed[0:number_of // 2 * 2:2], mixed[1:number_of // 2 * 2:2]
    room = jnp.minimum(sizes[giver] - 1, reach - sizes[receiver]) // 2
    room = jnp.where((giver == order[0]) | (receiver == order[0]) | (sizes[receiver] == 0), 0, jnp.maximum(room, 0))
    moved = jax.random.randint(jax.random.fold_in(own, 4), (number_of // 2,), 0, 1 << 20) % (room + 1)
    sizes = sizes.at[giver].add(-moved).at[receiver].add(moved)
    labels = jnp.searchsorted(jnp.cumsum(sizes), jnp.arange(rows * top), side="right").astype(jnp.int32)
    grid = labels.reshape(top, rows).T
    grid = grid[jax.random.permutation(jax.random.fold_in(own, 1), rows)]
    turn = jax.random.randint(jax.random.fold_in(own, 2), (rows, 1), 0, top)
    return jnp.take_along_axis(grid, (jnp.arange(top)[None, :] + turn) % top, axis=1)


def load_shares(count, total, limit, skew, full):
    weights = [(1 << 20) // math.isqrt(rank ** skew) + 1 for rank in range(1, count + 1)]
    largest = limit if full else min(limit, max(-(-total // count), total * weights[0] // sum(weights)))
    least = 1 if total - largest >= count - 1 else 0
    holding, surplus = [largest] + [least] * (count - 1), total - largest - least * (count - 1)
    while surplus > 0:
        movable = [i for i in range(1, count) if holding[i] < largest] or [i for i in range(1, count) if holding[i] < limit]
        whole, left = sum([weights[i] for i in movable]), surplus
        for i in movable:
            more = min(limit - holding[i], max(1, left * weights[i] // whole), surplus)
            holding[i] = holding[i] + more
            surplus = surplus - more
    return np.array(holding)


def noise(key, extent, deviation, reach, shards=(), kind=jnp.bfloat16):
    drawn = jax.random.normal(key, extent, jnp.float32) * deviation
    if len(shards) > 0:
        drawn = steps_of(key, extent, shards, -0.22, 0.18) * drawn
    return jnp.clip(drawn, min=-reach, max=reach).astype(kind)


def setup_inputs(seed: int = 0) -> dict:
    seeds = jax.random.split(jax.random.key(seed), 10)
    queries = noise(seeds[0], (LENGTH, HEADS * DH), 1.0, 6.0, ((0, 4), (1, 8)), jnp.float32)
    key_rows = noise(seeds[1], (LENGTH, HEADS * DH), 1.0, 6.0, ((0, 4), (1, 8)), jnp.float32)
    values = noise(seeds[2], (LENGTH, HEADS * DH), 1.0, 6.0, ((0, 4), (1, 8)), jnp.float32)
    out_weight = noise(seeds[3], (HEADS * DH, D), (HEADS * DH) ** -0.5, 0.09375, ((0, 8),))
    expert_ids_keys = jax.random.split(jax.random.fold_in(seeds[4], 1), TOKENS // TOK_DEV)
    expert_ids_turns = jax.random.permutation(jax.random.fold_in(seeds[4], 3), TOKENS // TOK_DEV)
    expert_ids = jax.vmap(lambda own, number: deal_out(jax.random.fold_in(seeds[4], 2), own, number, TOK_DEV, EXPERTS, TOP, CAP, 2))(expert_ids_keys, expert_ids_turns).reshape((TOKENS, TOP))
    gate_ints = set_ends(jax.random.randint(seeds[5], (TOKENS, TOP), 1, 1024), jax.random.fold_in(seeds[5], 1), 1, 1023).astype(jnp.int32)
    w_gate = noise(seeds[6], (EXPERTS, D, FF), D ** -0.5, 0.125, ((0, 32),))
    w_up = noise(seeds[7], (EXPERTS, D, FF), D ** -0.5, 0.125, ((0, 32),))
    w_down = noise(seeds[8], (EXPERTS, FF, D), FF ** -0.5, 0.21875, ((0, 32),))
    return {"queries": queries, "key_rows": key_rows, "values": values, "out_weight": out_weight, "expert_ids": expert_ids, "gate_ints": gate_ints, "w_gate": w_gate, "w_up": w_up, "w_down": w_down}


HIGH = lax.Precision.HIGHEST

def causal_linear(query_heads, key_heads, value_heads):
    heads, length, width = query_heads.shape
    block = math.gcd(512, length)
    count = length // block

    def split(array):
        return array.reshape(heads, count, block, width).transpose(1, 0, 2, 3)
    lower = jnp.tril(jnp.ones((block, block), jnp.float32))

    def advance(state, inputs):
        query_block, key_block, value_block = inputs
        scores = jnp.einsum('hid,hjd->hij', query_block, key_block, precision=HIGH) * lower
        output = jnp.einsum('hij,hjd->hid', scores, value_block, precision=HIGH)
        output = output + jnp.einsum('hid,hde->hie', query_block, state, precision=HIGH)
        state = state + jnp.einsum('hjd,hje->hde', key_block, value_block, precision=HIGH)
        return (state, output)
    start = jnp.zeros((heads, width, width), jnp.float32)
    state, outputs = lax.scan(advance, start, (split(query_heads), split(key_heads), split(value_heads)))
    return (outputs.transpose(1, 0, 2, 3).reshape(heads, length, width), state)

def head_norm(mixed):
    return mixed * lax.rsqrt(lax.optimization_barrier(jnp.mean(mixed * mixed, axis=-1, keepdims=True)) + 1e-06)

def reference(queries, key_rows, values, out_weight, expert_ids, gate_ints, w_gate, w_up, w_down):
    length = queries.shape[0]

    def split_heads(array):
        return array.reshape(length, HEADS, DH).transpose(1, 0, 2)
    heads_out, final_state = causal_linear(split_heads(queries), split_heads(key_rows), split_heads(values))
    attn = head_norm(heads_out).transpose(1, 0, 2).reshape(length, HEADS * DH).astype(jnp.bfloat16)
    projected = jnp.dot(attn, out_weight, preferred_element_type=jnp.float32)
    normed = (projected * lax.rsqrt(lax.optimization_barrier(jnp.mean(projected * projected, axis=-1, keepdims=True)) + 1e-06)).astype(jnp.bfloat16)
    gates = gate_ints.astype(jnp.float32)
    gates = gates / lax.optimization_barrier(jnp.sum(gates, axis=-1, keepdims=True))
    flat_ids = expert_ids.reshape(-1)
    flat_gates = gates.reshape(-1)
    count_all = flat_ids.shape[0]
    owner = jnp.arange(count_all, dtype=jnp.int32) // TOP
    slots = CAP * N_SEQ * N_HEAD

    def expert_step(total, inputs):
        expert, gate_mat, up_mat, down_mat = inputs
        chosen = flat_ids == expert
        rank = jnp.cumsum(chosen.astype(jnp.int32), dtype=jnp.int32) - 1
        target = jnp.where(chosen, rank, slots).astype(jnp.int32)
        source = jnp.zeros((slots,), jnp.int32).at[target].set(jnp.arange(count_all, dtype=jnp.int32), mode='drop')
        filled = jnp.arange(slots, dtype=jnp.int32) < jnp.sum(chosen.astype(jnp.int32))
        tokens = owner[source]
        picked = normed[tokens]
        gate_val = jnp.dot(picked, gate_mat, preferred_element_type=jnp.float32)
        up_val = jnp.dot(picked, up_mat, preferred_element_type=jnp.float32)
        act = (jax.nn.silu(gate_val) * up_val).astype(jnp.bfloat16)
        result = jnp.dot(act, down_mat, preferred_element_type=jnp.float32).astype(jnp.bfloat16)
        result = lax.optimization_barrier(result).astype(jnp.float32)
        weight = jnp.where(filled, flat_gates[source], jnp.zeros_like(flat_gates[source]))
        return (total.at[tokens].add(result * weight[:, None]), None)
    moe_sum, unused = lax.scan(expert_step, jnp.zeros((length, D), jnp.float32), (jnp.arange(EXPERTS, dtype=jnp.int32), w_gate, w_up, w_down))
    return projected + moe_sum
```

```python
import math

import jax
import jax.numpy as jnp
from jax import lax
from jax.sharding import PartitionSpec as P

DH = 128

HIGH = lax.Precision.HIGH


def flip(array, bit):
    return lax.ppermute(array, "head", [(i, i ^ bit) for i in range(lax.axis_size("head"))])


def shift(array, step):
    n = lax.axis_size("seq")
    return lax.ppermute(array, "seq", [(i, (i + step) % n) for i in range(n)])


def earlier_states(state):
    n = lax.axis_size("seq")
    sent = state.astype(jnp.bfloat16)
    total = jnp.zeros_like(state)
    for step in range(1, n):
        moved = lax.ppermute(sent, "seq", [(i, i + step) for i in range(n - step)])
        total = total + moved.astype(state.dtype)
    return total


def attention(queries, key_rows, values):
    length = queries.shape[0]
    heads = queries.shape[1] // DH

    def split_heads(array):
        return array.reshape(length, heads, DH).transpose(1, 0, 2)

    q, k, v = split_heads(queries), split_heads(key_rows), split_heads(values)
    state = jnp.einsum("hjd,hje->hde", k, v, precision=HIGH)
    before = earlier_states(state)
    block = math.gcd(512, length)
    lower = jnp.tril(jnp.ones((block, block), jnp.float32))
    outs = []
    for start in range(0, length, block):
        qb, kb, vb = (a[:, start : start + block] for a in (q, k, v))
        scores = jnp.einsum("hid,hjd->hij", qb, kb, precision=HIGH) * lower
        out = jnp.einsum("hij,hjd->hid", scores, vb, precision=HIGH)
        out = out + jnp.einsum("hid,hde->hie", qb, before, precision=HIGH)
        outs.append(out)
        if start + block < length:
            before = before + jnp.einsum("hjd,hje->hde", kb, vb, precision=HIGH)
    out = jnp.concatenate(outs, axis=1) if len(outs) > 1 else outs[0]
    out = out * lax.rsqrt(jnp.mean(out * out, axis=-1, keepdims=True) + 1e-06)
    return out.transpose(1, 0, 2).reshape(length, heads * DH).astype(jnp.bfloat16)


def project(attn, out_weight):
    length = attn.shape[0]
    count = lax.axis_size("head")
    here = lax.axis_index("head")
    blocks = attn.reshape(count, length // count, attn.shape[1])
    order = here ^ jnp.arange(count, dtype=jnp.int32)
    near = jnp.take(blocks, order[0::2], axis=0).reshape(length // 2, -1)
    far = jnp.take(blocks, order[1::2], axis=0).reshape(length // 2, -1)
    far = jnp.dot(far, out_weight, preferred_element_type=jnp.float32).astype(jnp.bfloat16)
    far = flip(far, 1)
    near = jnp.dot(near, out_weight, preferred_element_type=jnp.float32)
    total = (near + far.astype(jnp.float32)).reshape(count // 2, length // count, -1)
    owned = total[0]
    for place in range(1, count // 2):
        owned = owned + flip(total[place].astype(jnp.bfloat16), 2 * place).astype(jnp.float32)
    return owned


def ranked(hit):
    size = hit.shape[-1]
    upper = (jnp.arange(size)[:, None] < jnp.arange(size)[None, :]).astype(jnp.bfloat16)
    return jnp.dot(hit.astype(jnp.bfloat16), upper, preferred_element_type=jnp.float32).astype(jnp.int32)


def routing(expert_ids, gates, capacity):
    seqs, heads = lax.axis_size("seq"), lax.axis_size("head")
    z, h = lax.axis_index("seq"), lax.axis_index("head")
    expert = z * heads + h
    all_ids = lax.all_gather(expert_ids, ("seq", "head"))
    all_gates = lax.all_gather(gates, ("seq", "head"))
    match = all_ids == expert
    hit = jnp.any(match, axis=-1)
    weight = jnp.sum(jnp.where(match, all_gates, 0.0), axis=-1)
    places = jnp.arange(heads, dtype=jnp.int32)[:, None]
    steps = jnp.arange(seqs, dtype=jnp.int32)[None, :]
    source = (jnp.mod(z - steps, seqs) * heads + (h ^ places)).reshape(-1)
    hit, weight = hit[source], weight[source]
    rank = ranked(hit)
    slots = jnp.arange(capacity, dtype=jnp.int32)
    pick = (rank[:, None, :] == slots[None, :, None]) & hit[:, None, :]
    slot_gate = jnp.sum(jnp.where(pick, weight[:, None, :], 0.0), axis=-1)
    return pick.astype(jnp.bfloat16), slot_gate


def spread(own):
    seqs, heads = lax.axis_size("seq"), lax.axis_size("head")
    column = [own] + [shift(own, step) for step in range(1, seqs)]
    half = seqs // 2
    parts = [jnp.concatenate(column[:half], axis=0), jnp.concatenate(column[half:], axis=0)]
    bits = []
    bit = 2
    while bit < heads:
        bits.append(bit)
        bit *= 2
    held = [{0: parts[0]}, {0: parts[1]}]
    for side, order in enumerate((bits, bits[::-1])):
        for bit in order:
            for place in sorted(held[side]):
                held[side][place | bit] = flip(held[side][place], bit)
    for side in range(2):
        for place in sorted(held[side]):
            held[side][place | 1] = flip(held[side][place], 1)
    return [jnp.concatenate([held[0][p], held[1][p]], axis=0) for p in range(heads)]


def add(a, b):
    return (a.astype(jnp.float32) + b.astype(jnp.float32)).astype(jnp.bfloat16)


def collect(columns, rows):
    seqs, heads = lax.axis_size("seq"), lax.axis_size("head")
    for place in range(0, heads, 2):
        columns[place] = add(columns[place], flip(columns[place | 1], 1))
    half = rows * (seqs // 2)
    held = [{p: columns[p][:half] for p in range(0, heads, 2)}, {p: columns[p][half:] for p in range(0, heads, 2)}]
    bits = []
    bit = 2
    while bit < heads:
        bits.append(bit)
        bit *= 2
    for side, order in enumerate((bits, bits[::-1])):
        for bit in order:
            for place in sorted(held[side], reverse=True):
                if place & bit:
                    moved = flip(held[side].pop(place), bit)
                    held[side][place ^ bit] = add(held[side][place ^ bit], moved)
    column = jnp.concatenate([held[0][0], held[1][0]], axis=0)
    total = column[:rows].astype(jnp.float32)
    for step in range(1, seqs):
        total = total + shift(column[step * rows : (step + 1) * rows], -step).astype(jnp.float32)
    return total


def experts_by_gather(normed, expert_ids, gates, w_gate, w_up, w_down, capacity):
    rows, width = normed.shape
    pick, slot_gate = routing(expert_ids, gates, capacity)
    heads = lax.axis_size("head")
    seqs = lax.axis_size("seq")
    columns = spread(normed)
    blocks = jnp.stack(columns).reshape(heads * seqs, rows, width)
    picked = jnp.einsum("nct,ntd->ncd", pick, blocks, preferred_element_type=jnp.float32)
    picked = picked.astype(jnp.bfloat16).reshape(-1, width)
    gate_val = jnp.dot(picked, w_gate[0], preferred_element_type=jnp.float32)
    up_val = jnp.dot(picked, w_up[0], preferred_element_type=jnp.float32)
    act = (jax.nn.silu(gate_val) * up_val).astype(jnp.bfloat16)
    result = jnp.dot(act, w_down[0], preferred_element_type=jnp.float32)
    result = (result * slot_gate.reshape(-1)[:, None]).astype(jnp.bfloat16)
    result = result.reshape(heads * seqs, capacity, width)
    back = jnp.einsum("nct,ncd->ntd", pick, result, preferred_element_type=jnp.float32)
    back = back.astype(jnp.bfloat16).reshape(heads, seqs * rows, width)
    return collect([back[p] for p in range(heads)], rows)


def experts_by_exchange(normed, expert_ids, gates, w_gate, w_up, w_down, capacity):
    tok_count, width = normed.shape
    top_count = expert_ids.shape[1]
    local_experts = w_gate.shape[0]
    devices = lax.axis_size("seq") * lax.axis_size("head")
    experts = local_experts * devices
    flat_ids = expert_ids.reshape(-1)
    assigned = flat_ids.shape[0]
    onehot = (flat_ids[:, None] == jnp.arange(experts, dtype=jnp.int32)[None, :]).astype(jnp.int32)
    before_count = jnp.cumsum(onehot, axis=0, dtype=jnp.int32) - onehot
    position = jnp.sum(before_count * onehot, axis=1, dtype=jnp.int32)
    slot_index = flat_ids * capacity + position
    source = (
        jnp.zeros((experts * capacity,), jnp.int32)
        .at[slot_index]
        .set(jnp.arange(assigned, dtype=jnp.int32))
    )
    filled = jnp.zeros((experts * capacity,), jnp.bool_).at[slot_index].set(True)
    picked = normed[source // top_count]
    outgoing = jnp.where(filled[:, None], picked, jnp.zeros_like(picked))

    def exchange(array):
        return lax.all_to_all(array, ("seq", "head"), split_axis=0, concat_axis=0, tiled=True)

    received = exchange(outgoing.reshape(devices, local_experts, capacity, width))
    gate_val = jnp.einsum("nesd,edf->nesf", received, w_gate, preferred_element_type=jnp.float32)
    up_val = jnp.einsum("nesd,edf->nesf", received, w_up, preferred_element_type=jnp.float32)
    act = (jax.nn.silu(gate_val) * up_val).astype(jnp.bfloat16)
    result = jnp.einsum("nesf,efd->nesd", act, w_down, preferred_element_type=jnp.float32)
    returned = exchange(result.astype(jnp.bfloat16)).reshape(experts * capacity, width)
    gathered = returned[slot_index].astype(jnp.float32) * gates.reshape(-1)[:, None]
    return jnp.sum(gathered.reshape(tok_count, top_count, width), axis=1)


def shards(queries, key_rows, values, out_weight, expert_ids, gate_ints, w_gate, w_up, w_down):
    projected = project(attention(queries, key_rows, values), out_weight)
    normed = (
        projected * lax.rsqrt(jnp.mean(projected * projected, axis=-1, keepdims=True) + 1e-06)
    ).astype(jnp.bfloat16)
    gates = gate_ints.astype(jnp.float32)
    gates = gates / jnp.sum(gates, axis=-1, keepdims=True)
    tok_count, top_count = expert_ids.shape
    local_experts = w_gate.shape[0]
    devices = lax.axis_size("seq") * lax.axis_size("head")
    experts = local_experts * devices
    capacity = max(2, 2 * tok_count * top_count // experts)
    dense = local_experts == 1 and tok_count <= 2 * capacity and lax.axis_size("seq") % 2 == 0
    layer = experts_by_gather if dense else experts_by_exchange
    return projected + layer(normed, expert_ids, gates, w_gate, w_up, w_down, capacity)


def solution(mesh):
    placed = (
        P("seq", "head"),
        P("seq", "head"),
        P("seq", "head"),
        P("head", None),
        P(("seq", "head"), None),
        P(("seq", "head"), None),
        P(("seq", "head"), None, None),
        P(("seq", "head"), None, None),
        P(("seq", "head"), None, None),
    )
    return jax.shard_map(
        shards, mesh=mesh, in_specs=placed, out_specs=P(("seq", "head"), None), check_vma=False
    )
```

```python
import functools
import math

import jax
import jax.numpy as jnp
from jax import lax
from jax.experimental import pallas as pl
from jax.experimental.pallas import tpu as pltpu
from jax.sharding import PartitionSpec as P


DH = 128

HIGH = lax.Precision.HIGH


def flip(array, bit):
    return lax.ppermute(array, "head", [(i, i ^ bit) for i in range(lax.axis_size("head"))])


def shift(array, step):
    n = lax.axis_size("seq")
    return lax.ppermute(array, "seq", [(i, (i + step) % n) for i in range(n)])


def earlier_states(state):
    n = lax.axis_size("seq")
    sent = state.astype(jnp.bfloat16)
    total = jnp.zeros_like(state)
    for step in range(1, n):
        moved = lax.ppermute(sent, "seq", [(i, i + step) for i in range(n - step)])
        total = total + moved.astype(state.dtype)
    return total


def attention(queries, key_rows, values):
    length = queries.shape[0]
    heads = queries.shape[1] // DH

    def split_heads(array):
        return array.reshape(length, heads, DH).transpose(1, 0, 2)

    q, k, v = split_heads(queries), split_heads(key_rows), split_heads(values)
    state = jnp.einsum("hjd,hje->hde", k, v, precision=HIGH)
    before = earlier_states(state)
    block = math.gcd(512, length)
    lower = jnp.tril(jnp.ones((block, block), jnp.float32))
    outs = []
    for start in range(0, length, block):
        qb, kb, vb = (a[:, start : start + block] for a in (q, k, v))
        scores = jnp.einsum("hid,hjd->hij", qb, kb, precision=HIGH) * lower
        out = jnp.einsum("hij,hjd->hid", scores, vb, precision=HIGH)
        out = out + jnp.einsum("hid,hde->hie", qb, before, precision=HIGH)
        outs.append(out)
        if start + block < length:
            before = before + jnp.einsum("hjd,hje->hde", kb, vb, precision=HIGH)
    out = jnp.concatenate(outs, axis=1) if len(outs) > 1 else outs[0]
    out = out * lax.rsqrt(jnp.mean(out * out, axis=-1, keepdims=True) + 1e-06)
    return out.transpose(1, 0, 2).reshape(length, heads * DH).astype(jnp.bfloat16)


def project(attn, out_weight):
    length = attn.shape[0]
    count = lax.axis_size("head")
    here = lax.axis_index("head")
    blocks = attn.reshape(count, length // count, attn.shape[1])
    order = here ^ jnp.arange(count, dtype=jnp.int32)
    near = jnp.take(blocks, order[0::2], axis=0).reshape(length // 2, -1)
    far = jnp.take(blocks, order[1::2], axis=0).reshape(length // 2, -1)
    far = jnp.dot(far, out_weight, preferred_element_type=jnp.float32).astype(jnp.bfloat16)
    far = flip(far, 1)
    near = jnp.dot(near, out_weight, preferred_element_type=jnp.float32)
    total = (near + far.astype(jnp.float32)).reshape(count // 2, length // count, -1)
    owned = total[0]
    for place in range(1, count // 2):
        owned = owned + flip(total[place].astype(jnp.bfloat16), 2 * place).astype(jnp.float32)
    return owned


def pack(normed, expert_ids, gate_ints):
    top = expert_ids.shape[1]
    base = 32
    info = jnp.concatenate([expert_ids, gate_ints // base, gate_ints % base], axis=1)
    info = jnp.pad(info.astype(jnp.bfloat16), ((0, 0), (0, 128 - 3 * top)))
    return jnp.concatenate([normed, info], axis=1)


def expert_body(rows, top, capacity, count, expert_ref, *refs):
    pieces, weights, outs = refs[:count], refs[count : count + 3], refs[count + 3 : 2 * count + 3]
    held, w_gate, w_up, w_down, picked_ref, back_ref, piece_sem, weight_sem, out_sem = refs[2 * count + 3 :]
    size, width = outs[0].shape
    slots = size // rows * capacity
    loads = [pltpu.make_async_copy(piece, held.at[i], piece_sem.at[i]) for i, piece in enumerate(pieces)]
    fetch = [
        pltpu.make_async_copy(weight, kept, weight_sem.at[i])
        for i, (weight, kept) in enumerate(zip(weights, (w_gate, w_up, w_down)))
    ]
    for copy in loads + fetch:
        copy.start()
    expert = expert_ref[0].astype(jnp.float32)
    row = lax.broadcasted_iota(jnp.int32, (size, size), 0)
    col = lax.broadcasted_iota(jnp.int32, (size, size), 1)
    below = ((col < row) & (col // rows == row // rows)).astype(jnp.bfloat16)
    block = lax.broadcasted_iota(jnp.int32, (size, slots), 0) // rows
    slot = lax.broadcasted_iota(jnp.int32, (size, slots), 1)
    slot = (slot - block * capacity).astype(jnp.float32)
    picks, shares = [], []
    for place in range(count):
        loads[place].wait()
        info = held[place, :, width:].astype(jnp.float32)
        ids, gates = info[:, :top], info[:, top : 2 * top] * 32.0 + info[:, 2 * top : 3 * top]
        own = jnp.sum(jnp.where(ids == expert, gates, 0.0), axis=-1, keepdims=True)
        shares.append(own / jnp.sum(gates, axis=-1, keepdims=True))
        hit = jnp.broadcast_to((own > 0.0).astype(jnp.float32), (size, slots))
        rank = jnp.dot(below, hit.astype(jnp.bfloat16), preferred_element_type=jnp.float32)
        pick = jnp.where((rank == slot) & (hit > 0.0), 1.0, 0.0).astype(jnp.bfloat16)
        picks.append(pick)
        picked = lax.dot_general(
            pick, held[place, :, :width], (((0,), (0,)), ((), ())), preferred_element_type=jnp.float32
        )
        picked_ref[place * slots : (place + 1) * slots, :] = picked.astype(jnp.bfloat16)
    picked = picked_ref[...]
    fetch[0].wait()
    gate_val = jnp.dot(picked, w_gate[...], preferred_element_type=jnp.float32)
    gate_val = gate_val / (1.0 + jnp.exp(-gate_val))
    fetch[1].wait()
    up_val = jnp.dot(picked, w_up[...], preferred_element_type=jnp.float32)
    act = (gate_val * up_val).astype(jnp.bfloat16)
    fetch[2].wait()
    stores = []
    for place in range(count):
        result = jnp.dot(
            act[place * slots : (place + 1) * slots], w_down[...], preferred_element_type=jnp.float32
        ).astype(jnp.bfloat16)
        back = jnp.dot(picks[place], result, preferred_element_type=jnp.float32)
        back_ref[place] = (back * shares[place]).astype(jnp.bfloat16)
        stores.append(pltpu.make_async_copy(back_ref.at[place], outs[place], out_sem.at[place]))
        stores[-1].start()
    for copy in stores:
        copy.wait()


def expert_call(pieces, expert, weights, rows, top, capacity):
    size, packed = pieces[0].shape
    count, width = len(pieces), packed - 128
    slots = size // rows * capacity * count
    hidden = weights[0].shape[1]
    anywhere = pl.BlockSpec(memory_space=pl.ANY)
    bf = jnp.bfloat16
    return pl.pallas_call(
        functools.partial(expert_body, rows, top, capacity, count),
        in_specs=[pl.BlockSpec(memory_space=pltpu.SMEM)] + [anywhere] * (count + 3),
        out_specs=[anywhere] * count,
        out_shape=[jax.ShapeDtypeStruct((size, width), bf)] * count,
        scratch_shapes=[
            pltpu.VMEM((count, size, packed), bf),
            pltpu.VMEM((width, hidden), bf),
            pltpu.VMEM((width, hidden), bf),
            pltpu.VMEM((hidden, width), bf),
            pltpu.VMEM((slots, width), bf),
            pltpu.VMEM((count, size, width), bf),
            pltpu.SemaphoreType.DMA((count,)),
            pltpu.SemaphoreType.DMA((3,)),
            pltpu.SemaphoreType.DMA((count,)),
        ],
        cost_estimate=pl.CostEstimate(
            flops=6 * slots * width * hidden,
            transcendentals=slots * hidden,
            bytes_accessed=6 * width * hidden + 4 * size * width * count,
        ),
    )(expert, *pieces, *weights)


def spread(own):
    seqs, heads = lax.axis_size("seq"), lax.axis_size("head")
    column = [own] + [shift(own, step) for step in range(1, seqs)]
    half = seqs // 2
    parts = [jnp.concatenate(column[:half], axis=0), jnp.concatenate(column[half:], axis=0)]
    bits = ici_bits(heads)
    held = [{0: parts[0]}, {0: parts[1]}]
    for side, order in enumerate((bits, bits[::-1])):
        for bit in order:
            for place in sorted(held[side]):
                held[side][place | bit] = flip(held[side][place], bit)
    for side in range(2):
        for place in sorted(held[side]):
            held[side][place | 1] = flip(held[side][place], 1)
    return held


def ici_bits(heads):
    bits = []
    bit = 2
    while bit < heads:
        bits.append(bit)
        bit *= 2
    return bits


def add(a, b):
    return (a.astype(jnp.float32) + b.astype(jnp.float32)).astype(jnp.bfloat16)


def collect(sent, rows):
    seqs, heads = lax.axis_size("seq"), lax.axis_size("head")
    bits = ici_bits(heads)
    parts = []
    for side, order in enumerate((bits, bits[::-1])):
        held = {}
        for p in range(0, heads, 2):
            held[p] = add(sent[side][p], flip(sent[side][p | 1], 1))
        for bit in order:
            for place in sorted(held):
                if place & bit:
                    moved = flip(held.pop(place), bit)
                    held[place ^ bit] = add(held[place ^ bit], moved)
        parts += [held[0][i : i + rows] for i in range(0, held[0].shape[0], rows)]
    total = parts[0].astype(jnp.float32)
    for step in range(1, seqs):
        total = total + shift(parts[step], -step).astype(jnp.float32)
    return total


def experts_by_gather(normed, expert_ids, gate_ints, w_gate, w_up, w_down, capacity):
    rows, top = expert_ids.shape
    heads = lax.axis_size("head")
    expert = (lax.axis_index("seq") * heads + lax.axis_index("head")).astype(jnp.int32).reshape(1)
    held = spread(pack(normed, expert_ids, gate_ints))
    weights = (w_gate[0], w_up[0], w_down[0])
    sent = [{}, {}]
    single = [p for p in range(heads) if (p >> 1).bit_count() == 1]
    others = [p for p in range(heads) if p not in single]
    for places in (single, others):
        keys = [(side, p) for p in places for side in range(2)]
        outs = expert_call([held[side][p] for side, p in keys], expert, weights, rows, top, capacity)
        for (side, p), out in zip(keys, outs):
            sent[side][p] = out
    return collect(sent, rows)


def experts_by_exchange(normed, expert_ids, gate_ints, w_gate, w_up, w_down, capacity):
    gates = gate_ints.astype(jnp.float32)
    gates = gates / jnp.sum(gates, axis=-1, keepdims=True)
    tok_count, width = normed.shape
    top_count = expert_ids.shape[1]
    local_experts = w_gate.shape[0]
    devices = lax.axis_size("seq") * lax.axis_size("head")
    experts = local_experts * devices
    flat_ids = expert_ids.reshape(-1)
    assigned = flat_ids.shape[0]
    onehot = (flat_ids[:, None] == jnp.arange(experts, dtype=jnp.int32)[None, :]).astype(jnp.int32)
    before_count = jnp.cumsum(onehot, axis=0, dtype=jnp.int32) - onehot
    position = jnp.sum(before_count * onehot, axis=1, dtype=jnp.int32)
    slot_index = flat_ids * capacity + position
    source = (
        jnp.zeros((experts * capacity,), jnp.int32)
        .at[slot_index]
        .set(jnp.arange(assigned, dtype=jnp.int32))
    )
    filled = jnp.zeros((experts * capacity,), jnp.bool_).at[slot_index].set(True)
    picked = normed[source // top_count]
    outgoing = jnp.where(filled[:, None], picked, jnp.zeros_like(picked))

    def exchange(array):
        return lax.all_to_all(array, ("seq", "head"), split_axis=0, concat_axis=0, tiled=True)

    received = exchange(outgoing.reshape(devices, local_experts, capacity, width))
    gate_val = jnp.einsum("nesd,edf->nesf", received, w_gate, preferred_element_type=jnp.float32)
    up_val = jnp.einsum("nesd,edf->nesf", received, w_up, preferred_element_type=jnp.float32)
    act = (jax.nn.silu(gate_val) * up_val).astype(jnp.bfloat16)
    result = jnp.einsum("nesf,efd->nesd", act, w_down, preferred_element_type=jnp.float32)
    returned = exchange(result.astype(jnp.bfloat16)).reshape(experts * capacity, width)
    gathered = returned[slot_index].astype(jnp.float32) * gates.reshape(-1)[:, None]
    return jnp.sum(gathered.reshape(tok_count, top_count, width), axis=1)


def layer_of(queries, key_rows, values, out_weight, expert_ids, gate_ints, w_gate, w_up, w_down):
    projected = project(attention(queries, key_rows, values), out_weight)
    normed = (
        projected * lax.rsqrt(jnp.mean(projected * projected, axis=-1, keepdims=True) + 1e-06)
    ).astype(jnp.bfloat16)
    tok_count, top_count = expert_ids.shape
    local_experts = w_gate.shape[0]
    devices = lax.axis_size("seq") * lax.axis_size("head")
    experts = local_experts * devices
    capacity = max(2, 2 * tok_count * top_count // experts)
    dense = local_experts == 1 and tok_count <= 2 * capacity and lax.axis_size("seq") % 2 == 0
    layer = experts_by_gather if dense else experts_by_exchange
    return projected + layer(normed, expert_ids, gate_ints, w_gate, w_up, w_down, capacity)


def solution(mesh):
    placed = (
        P("seq", "head"),
        P("seq", "head"),
        P("seq", "head"),
        P("head", None),
        P(("seq", "head"), None),
        P(("seq", "head"), None),
        P(("seq", "head"), None, None),
        P(("seq", "head"), None, None),
        P(("seq", "head"), None, None),
    )
    return jax.shard_map(
        layer_of, mesh=mesh, in_specs=placed, out_specs=P(("seq", "head"), None), check_vma=False
    )
```
